1024 devices in a mesh: gx: 16 (over z, core), gy: 8 (over x), gz: 8 (over y).
Axes of the slice: x: 8, y: 8, z: 8, core: 2. Of those that a mesh axis runs over, the one named last changes fastest.
Arguments:
- right_side: bfloat16 [64, 1024, 1024], P('gz', 'gx', 'gy'), may hold values from -6 to 6
- phase_mask: int32 [64, 1024, 1024], P('gz', 'gx', 'gy'), may hold values from 0 to 1, as said below
Outputs:
- pressure: float32 [64, 1024, 1024], P('gz', 'gx', 'gy')
- scaled_residual: float32 [64, 1024, 1024], P('gz', 'gx', 'gy')
The draws below stay inside these ranges and needn't reach their ends.
Inputs may be any that keep to these rules, and one draw needn't show every extreme that they name: `phase_mask`: 0 for a gas cell, 1 for a liquid cell.
All inputs are finite; a program needn't handle non-finite values.
Results may differ from the reference program's by a relative error of at most 0.0004.
Values may be sent and summed in bfloat16 or wider, within the bound.
A program may use at most 32 MiB of HBM per device.

```python
import math
import jax
import jax.numpy as jnp

ITERS = 3
NZ = 64
NX = 1024
NY = 1024


def draw_right_side(key, part):
    k_noise, k_phase, k_amp = jax.random.split(jax.random.fold_in(key, 11), 3)
    zpos = jnp.arange(NZ, dtype=jnp.float32)[:, None, None] / NZ
    xpos = jnp.arange(NX, dtype=jnp.float32)[None, :, None] / NX
    ypos = jnp.arange(NY, dtype=jnp.float32)[None, None, :] / NY
    phases = jax.random.uniform(k_phase, (4,), jnp.float32, -math.pi, math.pi)
    amps = jax.random.uniform(k_amp, (4,), jnp.float32, 0.5, 1.0)
    turn = 2.0 * math.pi
    smooth = amps[0] * jnp.sin(turn * xpos + phases[0])
    smooth = smooth + amps[1] * jnp.sin(turn * ypos + phases[1])
    smooth = smooth + amps[2] * jnp.sin(turn * zpos + phases[2])
    smooth = smooth + amps[3] * jnp.sin(turn * (xpos + ypos) + phases[3])
    noise = jax.random.normal(k_noise, (NZ, NX, NY), jnp.float32)
    return jnp.clip(noise + smooth, -6.0, 6.0).astype(jnp.bfloat16)


def draw_phase_mask(key, part):
    k_low, k_high, k_cell = jax.random.split(jax.random.fold_in(key, 7), 3)
    lower = jax.random.randint(k_low, (), 100, 301, jnp.int32)
    upper = jax.random.randint(k_high, (), 400, 701, jnp.int32)
    zindex = jnp.arange(NZ, dtype=jnp.int32)[:, None, None]
    xindex = jnp.arange(NX, dtype=jnp.int32)[None, :, None]
    ramp = (upper - lower) * (xindex * NZ + zindex * NX) // (2 * NX * NZ)
    threshold = lower + ramp
    cells = jax.random.randint(k_cell, (NZ, NX, NY), 0, 1000, jnp.int32)
    return (cells < threshold).astype(jnp.int32)


def setup_inputs(seed: int = 0) -> dict:
    key_of = jax.random.split(jax.random.key(seed), 3)
    right_side = draw_right_side(jax.random.fold_in(key_of[2], 71), 0)
    phase_mask = draw_phase_mask(jax.random.fold_in(key_of[2], 71), 0)
    return dict(right_side=right_side, phase_mask=phase_mask)


density_ratio = 1000.0
mass_shift = 0.05


def coupling(density, axis, offset):
    return 2.0 / (density + jnp.roll(density, offset, axis))


def operate(field, density):
    total = mass_shift * field
    for axis in range(3):
        for offset in (1, -1):
            total = total + coupling(density, axis, offset) * (field - jnp.roll(field, offset, axis))
    return total


def reference(right_side, phase_mask):
    density = 1.0 + (density_ratio - 1.0) * phase_mask.astype(jnp.float32)
    diagonal = jnp.full(density.shape, mass_shift, jnp.float32)
    for axis in range(3):
        for offset in (1, -1):
            diagonal = diagonal + coupling(density, axis, offset)
    source = diagonal * right_side.astype(jnp.float32)
    pressure = jnp.zeros_like(source)
    residual = source
    smoothed = residual / diagonal
    direction = smoothed
    energy = jnp.sum(residual * smoothed)
    for iteration in range(ITERS):
        applied = operate(direction, density)
        step_size = energy / jnp.sum(direction * applied)
        pressure = pressure + step_size * direction
        residual = residual - step_size * applied
        smoothed = residual / diagonal
        energy_next = jnp.sum(residual * smoothed)
        direction = smoothed + (energy_next / energy) * direction
        energy = energy_next
    return pressure, residual / diagonal
```

```python
import functools

import jax
import jax.numpy as jnp
from jax import lax
from jax.experimental import pallas as pl
from jax.experimental.pallas import tpu as pltpu
from jax.sharding import PartitionSpec as P

MESH = pl.DeviceIdType.MESH
F32 = jnp.float32
BF16 = jnp.bfloat16

mass_shift = 0.05
GAS = 1.0
MIXED = 2.0 / 1001.0
LIQUID = 0.001

NZ, NX, NY = 8, 64, 128
PAD = 16
ROWS = NX + 2 * PAD
LO, HI = PAD - 8, PAD + NX + 8
R = slice(LO, HI)
OWN = slice(8, 8 + NX)


def halo_offsets():
    out = []
    for dz in (-1, 0, 1):
        for dx in (-1, 0, 1):
            for dy in (-1, 0, 1):
                if (dz, dx, dy) != (0, 0, 0):
                    out.append((dz, dx, dy))
    return out


def kernel(sizes, rhs_hbm, mask_hbm, p_ref, r_ref, maskv, edge, pack, left, right,
           v0, mk, wx, wy, wz, di, u1, u2, u3, mine, got, in_sem, hs, hr, rs, rr):
    gz, gx, gy = sizes
    iz, ix, iy = (lax.axis_index(a) for a in ("gz", "gx", "gy"))

    def device(dz, dx, dy):
        return {
            "gz": lax.rem(iz + (dz % gz), gz),
            "gx": lax.rem(ix + (dx % gx), gx),
            "gy": lax.rem(iy + (dy % gy), gy),
        }

    own_rows = pl.ds(PAD, NX)
    own_planes = pl.ds(3, NZ)
    load_mask = pltpu.make_async_copy(mask_hbm, maskv, in_sem.at[0])
    load_rhs = pltpu.make_async_copy(rhs_hbm, edge.at[own_planes, 0, own_rows, :], in_sem.at[1])
    load_mask.start()
    load_rhs.start()

    partners = set((dz % gz, dx % gx, dy % gy) for dz, dx, dy in halo_offsets())
    partners |= set((0, 0, o) for o in range(1, gy))
    partners |= set((o, 0, 0) for o in range(1, gz))
    partners |= set((0, o, 0) for o in range(1, gx))
    partners = sorted(partners)
    barrier = pltpu.get_barrier_semaphore()
    for offset in partners:
        pl.semaphore_signal(barrier, inc=1, device_id=device(*offset), device_id_type=MESH)

    lane = lax.broadcasted_iota(jnp.int32, (NX, NY), 1)
    load_mask.wait()
    load_rhs.wait()
    edge[own_planes, 1, own_rows, :] = maskv[...].astype(F32).astype(BF16)
    packed = jnp.zeros((NX, NY), F32)
    for z in range(NZ):
        values = edge[3 + z, 0, own_rows, :].astype(F32)
        phases = maskv[z].astype(F32)
        packed = jnp.where(lane // 8 == z, pltpu.roll(values, 4 + 8 * z, 1), packed)
        packed = jnp.where(lane // 8 == z + 8, pltpu.roll(phases, 68 + 8 * z, 1), packed)
    pack[...] = packed.astype(BF16)
    pl.semaphore_wait(barrier, len(partners))

    z_from = {1: pl.ds(8, 3), -1: pl.ds(3, 3), 0: own_planes}
    z_to = {1: pl.ds(0, 3), -1: pl.ds(11, 3), 0: own_planes}
    z2_from = {1: pl.ds(9, 2), -1: pl.ds(3, 2), 0: own_planes}
    z2_to = {1: pl.ds(1, 2), -1: pl.ds(11, 2), 0: own_planes}
    x_from = {1: pl.ds(PAD + NX - 16, 16), -1: pl.ds(PAD, 16), 0: own_rows}
    x_to = {1: pl.ds(0, 16), -1: pl.ds(PAD + NX, 16), 0: own_rows}
    q_from = {1: pl.ds(NX - 16, 16), -1: pl.ds(0, 16), 0: pl.ds(0, NX)}
    copies = []
    for i, (dz, dx, dy) in enumerate(halo_offsets()):
        if dy == 0 and dx == 0:
            src = edge.at[z_from[dz], :, own_rows, :]
            dst = edge.at[z_to[dz], :, own_rows, :]
        elif dy == 0:
            src = edge.at[z2_from[dz], :, x_from[dx], :]
            dst = edge.at[z2_to[dz], :, x_to[dx], :]
        else:
            src = pack.at[q_from[dx], :]
            dst = (left if dy == 1 else right).at[1 - dz, x_to[dx], :]
        copy = pltpu.make_async_remote_copy(
            src_ref=src, dst_ref=dst, send_sem=hs.at[i], recv_sem=hr.at[i],
            device_id=device(dz, dx, dy), device_id_type=MESH,
        )
        copies.append(((dz == 0, abs(dz) + abs(dx) + abs(dy)), copy))
    for _, copy in sorted(copies, key=lambda c: c[0]):
        copy.start()
    for _, copy in copies:
        copy.wait_recv()

    half = lax.broadcasted_iota(jnp.int32, (HI - LO, NY), 1)
    low = lax.rem(half, 8) < 4
    first, last = half == 0, half == NY - 1

    def fill(side, base):
        joined = jnp.where(
            low, left[side].astype(F32)[LO:HI], right[side].astype(F32)[LO:HI]
        )

        def body(i, _):
            z, turn = base + i, i if side == 1 else (i + NZ - 3 if side == 0 else i)
            v0[z, 0, R, :] = edge[z, 0].astype(F32)[LO:HI]
            mk[z, 0, R, :] = edge[z, 1].astype(F32)[LO:HI]
            v0[z, 1, R, :] = pltpu.roll(joined, lax.rem(252 - 8 * turn, 128), 1)
            mk[z, 1, R, :] = pltpu.roll(joined, lax.rem(188 - 8 * turn, 128), 1)
            return 0

        lax.fori_loop(0, 3 if side != 1 else NZ, body, 0)

    fill(0, 0)
    fill(1, 3)
    fill(2, 11)

    def ahead(main, side):
        a, b = pltpu.roll(main, NY - 1, 1), pltpu.roll(side, NY - 1, 1)
        return jnp.where(last, b, a), jnp.where(last, a, b)

    def behind(main, side):
        a, b = pltpu.roll(main, 1, 1), pltpu.roll(side, 1, 1)
        return jnp.where(first, b, a), jnp.where(first, a, b)

    def weight(a, b):
        total = a + b
        return jnp.where(total < 0.5, GAS, jnp.where(total < 1.5, MIXED, LIQUID)).astype(F32)

    up, down = slice(LO + 1, HI + 1), slice(LO - 1, HI - 1)

    def fold(values):
        return jnp.sum(values.reshape(NX // 8, 8, NY), axis=0)

    def z_weights(z, _):
        for t in (0, 1):
            wz[z, t, R, :] = weight(mk[z, t, R, :], mk[z + 1, t, R, :])
        return 0

    lax.fori_loop(0, 13, z_weights, 0)

    def weights(z, _):
        here = [mk[z, t, R, :] for t in (0, 1)]
        there = ahead(*here)
        wy_now = [weight(a, b) for a, b in zip(here, there)]
        wy_back = behind(*wy_now)
        for t in (0, 1):
            wx_now = weight(here[t], mk[z, t, up, :])
            wx_back = weight(here[t], mk[z, t, down, :])
            total = mass_shift + wz[z, t, R, :] + wz[z - 1, t, R, :] + wx_now + wx_back
            total = total + wy_now[t] + wy_back[t]
            wx[z, t, R, :] = wx_now
            wy[z, t, R, :] = wy_now[t]
            di[z, t, R, :] = 1.0 / total
        return 0

    lax.fori_loop(1, 13, weights, 0)

    def image(field, z, sides):
        here = [field[z, t, R, :] for t in (0, 1)]
        there = ahead(*here)
        flow = [wy[z, t, R, :] * (here[t] - there[t]) for t in (0, 1)]
        back = behind(*flow)
        out = []
        for t in sides:
            v = here[t]
            total = mass_shift * v + wz[z, t, R, :] * (v - field[z + 1, t, R, :])
            total = total + wz[z - 1, t, R, :] * (v - field[z - 1, t, R, :])
            total = total + wx[z, t, R, :] * (v - field[z, t, up, :])
            total = total + wx[z, t, down, :] * (v - field[z, t, down, :])
            out.append(total + (flow[t] - back[t]))
        return here[0], out

    def advance(field, result, low_z, high_z, sides):
        def body(z, sums):
            here, totals = image(field, z, sides)
            for t, total in zip(sides, totals):
                now = total * di[z, t, R, :]
                result[z, t, R, :] = now
                if t == 0:
                    scale = jnp.where((z >= 3) & (z < 11), 1.0, 0.0).astype(F32)
                    owned = totals[0][OWN]
                    sums = (
                        sums[0] + scale * fold(here[OWN] * owned),
                        sums[1] + scale * fold(now[OWN] * owned),
                    )
            return sums

        zero = jnp.zeros((8, NY), F32)
        return lax.fori_loop(low_z, high_z, body, (zero, zero))

    def start_energy(z, total):
        v = v0[z, 0, pl.ds(PAD, NX), :]
        return total + fold(v * v / di[z, 0, pl.ds(PAD, NX), :])

    m0 = lax.fori_loop(3, 11, start_energy, jnp.zeros((8, NY), F32))
    m1, m2 = advance(v0, u1, 1, 13, (0, 1))
    m3, m4 = advance(u1, u2, 2, 12, (0, 1))
    m5, _ = advance(u2, u3, 3, 11, (0,))

    spot = lax.broadcasted_iota(jnp.int32, (1, NY), 1)
    row = jnp.zeros((1, NY), F32)
    for k, m in enumerate((m0, m1, m2, m3, m4, m5)):
        row = jnp.where(spot == k, jnp.sum(m, keepdims=True), row)

    place = 0
    for turn, (axis, n) in enumerate((("gy", gy), ("gz", gz), ("gx", gx))):
        mine[turn] = row
        sent = []
        for o in range(1, n):
            step = {"gz": 0, "gx": 0, "gy": 0}
            step[axis] = o
            copy = pltpu.make_async_remote_copy(
                src_ref=mine.at[turn], dst_ref=got.at[place],
                send_sem=rs.at[place], recv_sem=rr.at[place],
                device_id=device(step["gz"], step["gx"], step["gy"]), device_id_type=MESH,
            )
            copy.start()
            sent.append((place, copy))
            place += 1
        for at, copy in sent:
            copy.wait_recv()
            row = row + got[at]
        copies += [((), copy) for _, copy in sent]

    m = [jnp.sum(jnp.where(spot == k, row, 0.0), axis=1, keepdims=True) for k in range(6)]

    def inner(a, b):
        total = None
        for i, ai in enumerate(a):
            for j, bj in enumerate(b):
                if ai is None or bj is None:
                    continue
                term = ai * bj * m[i + j]
                total = term if total is None else total + term
        return total

    one = jnp.ones((1, 1), F32)
    z_poly, p_poly, x_poly, energy = [one], [one], [], m[0]
    for it in range(3):
        q_poly = [None] + p_poly
        step_size = energy / inner(p_poly, q_poly)
        x_poly = [
            step_size * p if i >= len(x_poly) else x_poly[i] + step_size * p
            for i, p in enumerate(p_poly)
        ]
        z_poly = [
            -step_size * q if i >= len(z_poly) else z_poly[i] if q is None else z_poly[i] - step_size * q
            for i, q in enumerate(q_poly)
        ]
        if it < 2:
            energy_next = inner(z_poly, z_poly)
            factor = energy_next / energy
            p_poly = [
                z_poly[i] if i >= len(p_poly) else z_poly[i] + factor * p_poly[i]
                for i in range(len(z_poly))
            ]
            energy = energy_next

    def finish(z, _):
        basis = [f[z + 3, 0, pl.ds(PAD, NX), :] for f in (v0, u1, u2, u3)]
        p_ref[z] = x_poly[0] * basis[0] + x_poly[1] * basis[1] + x_poly[2] * basis[2]
        r_ref[z] = (
            z_poly[0] * basis[0] + z_poly[1] * basis[1] + z_poly[2] * basis[2] + z_poly[3] * basis[3]
        )
        return 0

    lax.fori_loop(0, NZ, finish, 0)
    for _, copy in copies:
        copy.wait_send()


def solution(mesh):
    sizes = (mesh.shape["gz"], mesh.shape["gx"], mesh.shape["gy"])
    hops = sum(sizes) - 3
    field = pltpu.VMEM((14, 2, ROWS, NY), F32)

    def on_device(right_side, phase_mask):
        block = jax.ShapeDtypeStruct((NZ, NX, NY), F32)
        return pl.pallas_call(
            functools.partial(kernel, sizes),
            out_shape=(block, block),
            in_specs=[pl.BlockSpec(memory_space=pl.ANY)] * 2,
            out_specs=[pl.BlockSpec(memory_space=pltpu.VMEM)] * 2,
            scratch_shapes=[
                pltpu.VMEM((NZ, NX, NY), jnp.int32),
                pltpu.VMEM((14, 2, ROWS, NY), BF16),
                pltpu.VMEM((NX, NY), BF16),
                pltpu.VMEM((3, ROWS, NY), BF16),
                pltpu.VMEM((3, ROWS, NY), BF16),
                *([field] * 9),
                pltpu.VMEM((3, 1, NY), F32),
                pltpu.VMEM((hops, 1, NY), F32),
                pltpu.SemaphoreType.DMA((2,)),
                pltpu.SemaphoreType.DMA((26,)),
                pltpu.SemaphoreType.DMA((26,)),
                pltpu.SemaphoreType.DMA((hops,)),
                pltpu.SemaphoreType.DMA((hops,)),
            ],
            compiler_params=pltpu.CompilerParams(collective_id=0, has_side_effects=True),
        )(right_side, phase_mask)

    placed = P("gz", "gx", "gy")
    return jax.shard_map(
        on_device, mesh=mesh, in_specs=(placed, placed), out_specs=(placed, placed), check_vma=False
    )
```

```python
import functools

import jax
import jax.numpy as jnp
from jax import lax
from jax.experimental import pallas as pl
from jax.experimental.pallas import tpu as pltpu
from jax.sharding import PartitionSpec as P

MESH = pl.DeviceIdType.MESH
F32 = jnp.float32
BF16 = jnp.bfloat16

mass_shift = 0.05
GAS = 1.0
MIXED = 2.0 / 1001.0
LIQUID = 0.001

NZ, NX, NY = 8, 64, 128
PAD = 16
ROWS = NX + 2 * PAD
LO, HI = PAD - 8, PAD + NX + 8
R = slice(LO, HI)
UP, DOWN = slice(LO + 1, HI + 1), slice(LO - 1, HI - 1)
OWN = slice(8, 8 + NX)


def halo_offsets():
    out = []
    for dz in (-1, 0, 1):
        for dx in (-1, 0, 1):
            for dy in (-1, 0, 1):
                if (dz, dx, dy) != (0, 0, 0):
                    out.append((dz, dx, dy))
    return out


def kernel(sizes, rhs_hbm, mask_hbm, b1, b2, b3, k0, k1, k2, k3, k4, k5, k6, maskv, edge, pack, left, right,
           v0, mk, wx, wy, wb, wz, di, u1, u2, u3, mine, got, in_sem, hs, hr, rs, rr, ready):
    gz, gx, gy = sizes
    iz, ix, iy = (lax.axis_index(a) for a in ("gz", "gx", "gy"))

    def device(dz, dx, dy):
        return {
            "gz": lax.rem(iz + (dz % gz), gz),
            "gx": lax.rem(ix + (dx % gx), gx),
            "gy": lax.rem(iy + (dy % gy), gy),
        }

    own_rows = pl.ds(PAD, NX)
    own_planes = pl.ds(3, NZ)
    load_mask = pltpu.make_async_copy(mask_hbm, maskv, in_sem.at[0])
    load_rhs = pltpu.make_async_copy(rhs_hbm, edge.at[own_planes, 0, own_rows, :], in_sem.at[1])
    load_mask.start()
    load_rhs.start()

    near = sorted(
        {(o % gz, 0, 0) for o in (1, -1)}
        | {(0, o % gx, 0) for o in (1, -1, 2, -2)}
        | {(0, 0, o % gy) for o in (1, -1)}
        - {(0, 0, 0)}
    )
    far = sorted(
        ({(o % gz, 0, 0) for o in (2, -2)}
        | {(0, o % gx, 0) for o in (4, -4)}
        | {(0, 0, o % gy) for o in (2, -2)})
        - {(0, 0, 0)}
    )

    def greet(semaphore, offsets):
        for offset in offsets:
            pl.semaphore_signal(semaphore, inc=1, device_id=device(*offset), device_id_type=MESH)

    barrier = pltpu.get_barrier_semaphore()
    greet(barrier, near)

    lane = lax.broadcasted_iota(jnp.int32, (NX, NY), 1)
    load_mask.wait()
    load_rhs.wait()
    edge[own_planes, 1, own_rows, :] = maskv[...].astype(F32).astype(BF16)
    packed = jnp.zeros((NX, NY), F32)
    for z in range(NZ):
        values = edge[3 + z, 0, own_rows, :].astype(F32)
        phases = maskv[z].astype(F32)
        packed = jnp.where(lane // 8 == z, pltpu.roll(values, 4 + 8 * z, 1), packed)
        packed = jnp.where(lane // 8 == z + 8, pltpu.roll(phases, 68 + 8 * z, 1), packed)
    pack[...] = packed.astype(BF16)
    pl.semaphore_wait(barrier, len(near))

    z_from = {1: pl.ds(8, 3), -1: pl.ds(3, 3), 0: own_planes}
    z_to = {1: pl.ds(0, 3), -1: pl.ds(11, 3), 0: own_planes}
    z2_from = {1: pl.ds(9, 2), -1: pl.ds(3, 2), 0: own_planes}
    z2_to = {1: pl.ds(1, 2), -1: pl.ds(11, 2), 0: own_planes}
    x_from = {1: pl.ds(PAD + NX - 16, 16), -1: pl.ds(PAD, 16), 0: own_rows}
    x_to = {1: pl.ds(0, 16), -1: pl.ds(PAD + NX, 16), 0: own_rows}
    q_from = {1: pl.ds(NX - 16, 16), -1: pl.ds(0, 16), 0: pl.ds(0, NX)}
    copies = []
    for dz, dx, dy in halo_offsets():
        if dy == 0 and dx == 0:
            src = edge.at[z_from[dz], :, own_rows, :]
            dst = edge.at[z_to[dz], :, own_rows, :]
        elif dy == 0:
            src = edge.at[z2_from[dz], :, x_from[dx], :]
            dst = edge.at[z2_to[dz], :, x_to[dx], :]
        else:
            src = pack.at[q_from[dx], :]
            dst = (left if dy == 1 else right).at[1 - dz, x_to[dx], :]
        copy = pltpu.make_async_remote_copy(
            src_ref=src, dst_ref=dst, send_sem=hs.at[0], recv_sem=hr.at[0 if dz == 0 else 1],
            device_id=device(dz, dx, dy), device_id_type=MESH,
        )
        copies.append((abs(dz) + abs(dx) + abs(dy), dz == 0, copy))
    for distance in (1, 2, 3):
        if distance > 1:
            greet(ready.at[distance - 2], near)
            pl.semaphore_wait(ready.at[distance - 2], len(near))
        for late in (False, True):
            for length, flat, copy in copies:
                if length == distance and flat == late:
                    copy.start()
    greet(ready.at[2], far)

    def settle(semaphore, ref):
        pltpu.make_async_copy(ref, ref, semaphore).wait()

    def arrived(early):
        settle(hr.at[0 if early else 1], v0.at[pl.ds(0, 11), 0, pl.ds(0, 32 if early else 64), :])

    half = lax.broadcasted_iota(jnp.int32, (1, NY), 1)
    low = lax.rem(half, 8) < 4
    first, last = half == 0, half == NY - 1

    def fill(side, base, count):
        joined = jnp.where(
            low, left[side].astype(F32)[LO:HI], right[side].astype(F32)[LO:HI]
        )

        def body(i, _):
            z = base + i
            turn = i + NZ - 3 if side == 0 else i
            v0[z, 0, R, :] = edge[z, 0].astype(F32)[LO:HI]
            mk[z, 0, R, :] = edge[z, 1].astype(F32)[LO:HI]
            v0[z, 1, R, :] = pltpu.roll(joined, lax.rem(252 - 8 * turn, 128), 1)
            mk[z, 1, R, :] = pltpu.roll(joined, lax.rem(188 - 8 * turn, 128), 1)
            return 0

        lax.fori_loop(0, count, body, 0, unroll=True)

    def ahead(main, side):
        a, b = pltpu.roll(main, NY - 1, 2), pltpu.roll(side, NY - 1, 2)
        return jnp.where(last, b, a), jnp.where(last, a, b)

    def behind(main, side):
        a, b = pltpu.roll(main, 1, 2), pltpu.roll(side, 1, 2)
        return jnp.where(first, b, a), jnp.where(first, a, b)

    def weight(a, b):
        total = a + b
        return jnp.where(total < 0.5, GAS, jnp.where(total < 1.5, MIXED, LIQUID)).astype(F32)

    def fold(values):
        return jnp.sum(values.reshape(NX // 8, 8, NY), axis=0)

    def weights(z, n, energy):
        here = [mk[pl.ds(z, n), t, R, :] for t in (0, 1)]
        after, before = ahead(*here), behind(*here)
        for t in (0, 1):
            across = weight(mk[pl.ds(z - 1, n + 1), t, R, :], mk[pl.ds(z, n + 1), t, R, :])
            wz[pl.ds(z - 1, n + 1), t, R, :] = across
            wx_now = weight(here[t], mk[pl.ds(z, n), t, UP, :])
            wx_back = weight(here[t], mk[pl.ds(z, n), t, DOWN, :])
            wy_now, wy_back = weight(here[t], after[t]), weight(here[t], before[t])
            total = mass_shift + across[1:] + across[:-1] + wx_now + wx_back + wy_now + wy_back
            wx[pl.ds(z, n), t, R, :] = wx_now
            wy[pl.ds(z, n), t, R, :] = wy_now
            wb[pl.ds(z, n), t, R, :] = wy_back
            di[pl.ds(z, n), t, R, :] = 1.0 / total
            if t == 0:
                v = v0[pl.ds(z, n), 0, R, :]
                for k in range(n):
                    scale = jnp.where((z + k >= 3) & (z + k < 11), 1.0, 0.0).astype(F32)
                    energy = energy + scale * fold((v[k] * v[k] * total[k])[OWN])
        return energy

    def image(field, z, n, sides, a, b):
        zs, rows = pl.ds(z, n), slice(a, b)
        here = [field[zs, t, rows, :] for t in (0, 1)]
        after, before = ahead(*here), behind(*here)
        out = []
        for t in sides:
            v = here[t]
            total = mass_shift * v
            total = total + wz[zs, t, rows, :] * (v - field[pl.ds(z + 1, n), t, rows, :])
            total = total + wz[pl.ds(z - 1, n), t, rows, :] * (v - field[pl.ds(z - 1, n), t, rows, :])
            total = total + wx[zs, t, rows, :] * (v - field[zs, t, a + 1 : b + 1, :])
            total = total + wx[zs, t, a - 1 : b - 1, :] * (v - field[zs, t, a - 1 : b - 1, :])
            total = total + wy[zs, t, rows, :] * (v - after[t])
            total = total + wb[zs, t, rows, :] * (v - before[t])
            out.append(total)
        return here[0], out

    def advance(field, result, groups, n, sums, ends=False):
        a, b = (PAD, PAD + NX) if ends else (LO, HI)
        inner_rows = slice(0, NX) if ends else OWN

        def body(i, sums):
            z = groups[0] + i * (groups[1] - groups[0]) if len(groups) > 1 else groups[0]
            here, totals = image(field, z, n, (0,) if ends else (0, 1), a, b)
            for t, total in enumerate(totals):
                now = total * di[pl.ds(z, n), t, a:b, :]
                result[pl.ds(z, n), t, a:b, :] = now
                if t == 0:
                    for k in range(n):
                        scale = jnp.where((z + k >= 3) & (z + k < 11), 1.0, 0.0).astype(F32)
                        owned = total[k][inner_rows]
                        sums = (
                            sums[0] + scale * fold(here[k][inner_rows] * owned),
                            sums[1] + scale * fold(now[k][inner_rows] * owned),
                        )
            return sums

        return lax.fori_loop(0, len(groups), body, sums)

    def lay(groups, n, energy):
        def body(i, energy):
            return weights(groups[0] + i * (groups[1] - groups[0]), n, energy)

        return lax.fori_loop(0, len(groups), body, energy)

    zero = jnp.zeros((8, NY), F32)
    s1 = s2 = s3 = (zero, zero)
    arrived(True)
    fill(1, 3, NZ)
    m0 = lay((4, 7), 3, zero)
    s1 = advance(v0, u1, (4, 7), 3, s1)
    s2 = advance(u1, u2, (5, 7), 2, s2)
    s3 = advance(u2, u3, (6,), 2, s3, True)
    arrived(False)
    fill(0, 0, 3)
    fill(2, 11, 3)
    m0 = lay((1, 10), 3, m0)
    s1 = advance(v0, u1, (1, 10), 3, s1)
    s2 = advance(u1, u2, (2, 9), 3, s2)
    s3 = advance(u2, u3, (3, 8), 3, s3, True)
    (m1, m2), (m3, m4), (m5, _) = s1, s2, s3

    spot = lax.broadcasted_iota(jnp.int32, (1, NY), 1)
    row = jnp.zeros((1, NY), F32)
    for k, m in enumerate((m0, m1, m2, m3, m4, m5)):
        row = jnp.where(spot == k, jnp.sum(m, keepdims=True), row)

    def keep(z, _):
        for out, field in ((b1, u1), (b2, u2), (b3, u3)):
            out[z] = field[z + 3, 0, pl.ds(PAD, NX), :]
        return 0

    pl.semaphore_wait(ready.at[2], len(far))
    place = 0
    for turn, (axis, n) in enumerate((("gy", gy), ("gz", gz), ("gx", gx))):
        mine[turn] = row
        for o in range(1, n):
            step = {"gz": 0, "gx": 0, "gy": 0}
            step[axis] = o
            pltpu.make_async_remote_copy(
                src_ref=mine.at[turn], dst_ref=got.at[place + o - 1],
                send_sem=rs.at[0], recv_sem=rr.at[turn],
                device_id=device(step["gz"], step["gx"], step["gy"]), device_id_type=MESH,
            ).start()
        if turn == 0:
            lax.fori_loop(0, NZ, keep, 0)
        settle(rr.at[turn], got.at[pl.ds(place, n - 1)])
        for o in range(1, n):
            row = row + got[place + o - 1]
        place += n - 1

    m = [jnp.sum(jnp.where(spot == k, row, 0.0), axis=1, keepdims=True) for k in range(6)]

    def inner(a, b):
        total = None
        for i, ai in enumerate(a):
            for j, bj in enumerate(b):
                if ai is None or bj is None:
                    continue
                term = ai * bj * m[i + j]
                total = term if total is None else total + term
        return total

    one = jnp.ones((1, 1), F32)
    z_poly, p_poly, x_poly, energy = [one], [one], [], m[0]
    for it in range(3):
        q_poly = [None] + p_poly
        step_size = energy / inner(p_poly, q_poly)
        x_poly = [
            step_size * p if i >= len(x_poly) else x_poly[i] + step_size * p
            for i, p in enumerate(p_poly)
        ]
        z_poly = [
            -step_size * q if i >= len(z_poly) else z_poly[i] if q is None else z_poly[i] - step_size * q
            for i, q in enumerate(q_poly)
        ]
        if it < 2:
            energy_next = inner(z_poly, z_poly)
            factor = energy_next / energy
            p_poly = [
                z_poly[i] if i >= len(p_poly) else z_poly[i] + factor * p_poly[i]
                for i in range(len(z_poly))
            ]
            energy = energy_next

    for out, c in zip((k0, k1, k2, k3, k4, k5, k6), x_poly + z_poly):
        out[...] = jnp.broadcast_to(c, (1, NY))
    settle(hs.at[0], v0.at[pl.ds(0, 11), 0])
    settle(rs.at[0], got)


def solution(mesh):
    sizes = (mesh.shape["gz"], mesh.shape["gx"], mesh.shape["gy"])
    hops = sum(sizes) - 3
    field = pltpu.VMEM((14, 2, ROWS, NY), F32)

    def on_device(right_side, phase_mask):
        block = jax.ShapeDtypeStruct((NZ, NX, NY), F32)
        coefficient = jax.ShapeDtypeStruct((1, NY), F32)
        u1, u2, u3, *coef = pl.pallas_call(
            functools.partial(kernel, sizes),
            out_shape=(block,) * 3 + (coefficient,) * 7,
            in_specs=[pl.BlockSpec(memory_space=pltpu.HBM)] * 2,
            out_specs=[pl.BlockSpec(memory_space=pltpu.VMEM)] * 10,
            scratch_shapes=[
                pltpu.VMEM((NZ, NX, NY), jnp.int32),
                pltpu.VMEM((14, 2, ROWS, NY), BF16),
                pltpu.VMEM((NX, NY), BF16),
                pltpu.VMEM((3, ROWS, NY), BF16),
                pltpu.VMEM((3, ROWS, NY), BF16),
                *([field] * 10),
                pltpu.VMEM((3, 1, NY), F32),
                pltpu.VMEM((hops, 1, NY), F32),
                pltpu.SemaphoreType.DMA((2,)),
                pltpu.SemaphoreType.DMA((1,)),
                pltpu.SemaphoreType.DMA((2,)),
                pltpu.SemaphoreType.DMA((1,)),
                pltpu.SemaphoreType.DMA((3,)),
                pltpu.SemaphoreType.REGULAR((3,)),
            ],
            compiler_params=pltpu.CompilerParams(
                collective_id=0, has_side_effects=True, vmem_limit_bytes=24 * 2**20
            ),
        )(*(pltpu.with_memory_space_constraint(a, pltpu.HBM) for a in (right_side, phase_mask)))
        u0 = right_side.astype(F32)
        c = [k[None] for k in coef]
        pressure = c[0] * u0 + c[1] * u1 + c[2] * u2
        return pressure, c[3] * u0 + c[4] * u1 + c[5] * u2 + c[6] * u3

    placed = P("gz", "gx", "gy")
    return jax.shard_map(
        on_device, mesh=mesh, in_specs=(placed, placed), out_specs=(placed, placed), check_vma=False
    )
```

```python
import functools

import jax
import jax.numpy as jnp
from jax import lax
from jax.experimental import pallas as pl
from jax.experimental.pallas import tpu as pltpu
from jax.sharding import PartitionSpec as P

MESH = pl.DeviceIdType.MESH
F32 = jnp.float32
BF16 = jnp.bfloat16

mass_shift = 0.05
HALF_GAS, HALF_STEP = 0.5, 499.5

NZ, NX, NY = 8, 64, 128
PAD = 16
ROWS = NX + 2 * PAD
LO, HI = PAD - 8, PAD + NX + 8
R = slice(LO, HI)
UP, DOWN = slice(LO + 1, HI + 1), slice(LO - 1, HI - 1)
OWN = slice(8, 8 + NX)


def halo_offsets():
    out = []
    for dz in (-1, 0, 1):
        for dx in (-1, 0, 1):
            for dy in (-1, 0, 1):
                if (dz, dx, dy) != (0, 0, 0):
                    out.append((dz, dx, dy))
    return out


def two_sum(a, b):
    s = a + b
    t = s - a
    return s, (a - (s - t)) + (b - t)


def quick(a, b):
    s = a + b
    return s, b - (s - a)


def split(a):
    c = 4097.0 * a
    high = c - (c - a)
    return high, a - high


def times(a, b):
    p = a[0] * b[0]
    (ah, al), (bh, bl) = split(a[0]), split(b[0])
    error = ((ah * bh - p) + ah * bl + al * bh) + al * bl
    return quick(p, error + (a[0] * b[1] + a[1] * b[0]))


def minus(a, b, c):
    p, e = times(b, c)
    s, t = two_sum(a[0], -p)
    return quick(s, t + (a[1] - e))


def kernel(sizes, rhs_hbm, mask_hbm, b1, b2, b3, k0, k1, k2, k3, k4, k5, k6, maskv, edge, pack, left, right,
           v0, mk, wx, wy, wb, wz, di, u1, u2, u3, mine, got, in_sem, hs, hr, rs, rr, ready):
    gz, gx, gy = sizes
    iz, ix, iy = (lax.axis_index(a) for a in ("gz", "gx", "gy"))

    def device(dz, dx, dy):
        return {
            "gz": lax.rem(iz + (dz % gz), gz),
            "gx": lax.rem(ix + (dx % gx), gx),
            "gy": lax.rem(iy + (dy % gy), gy),
        }

    own_rows = pl.ds(PAD, NX)
    own_planes = pl.ds(3, NZ)
    load_mask = pltpu.make_async_copy(mask_hbm, maskv, in_sem.at[0])
    load_rhs = pltpu.make_async_copy(rhs_hbm, edge.at[own_planes, 0, own_rows, :], in_sem.at[1])
    load_mask.start()
    load_rhs.start()

    near = sorted(
        {(o % gz, 0, 0) for o in (1, -1)}
        | {(0, o % gx, 0) for o in (1, -1, 2, -2)}
        | {(0, 0, o % gy) for o in (1, -1)}
        - {(0, 0, 0)}
    )
    far = sorted(
        ({(o % gz, 0, 0) for o in (2, -2)}
        | {(0, o % gx, 0) for o in (4, -4)}
        | {(0, 0, o % gy) for o in (2, -2)})
        - {(0, 0, 0)}
    )

    distant = sorted(({(o % gz, 0, 0) for o in (4, -4)} | {(0, 0, o % gy) for o in (4, -4)}) - {(0, 0, 0)})

    wide = sorted(
        set(near)
        | {
            (dz % gz, dx % gx, dy % gy)
            for dz, dx, dy in halo_offsets()
            if abs(dz) + abs(dx) + abs(dy) <= 2
        }
    )

    def reach(offset):
        return sum(min(o, n - o) for o, n in zip(offset, sizes))

    def greet(semaphore, offsets):
        for offset in offsets:
            pl.semaphore_signal(semaphore, inc=1, device_id=device(*offset), device_id_type=MESH)

    barrier = pltpu.get_barrier_semaphore()
    greet(barrier, wide)

    lane = lax.broadcasted_iota(jnp.int32, (NX, NY), 1)
    load_mask.wait()
    load_rhs.wait()
    edge[own_planes, 1, own_rows, :] = maskv[...].astype(F32).astype(BF16)
    packed = jnp.zeros((NX, NY), F32)
    for z in range(NZ):
        values = edge[3 + z, 0, own_rows, :].astype(F32)
        phases = maskv[z].astype(F32)
        packed = jnp.where(lane // 8 == z, pltpu.roll(values, 4 + 8 * z, 1), packed)
        packed = jnp.where(lane // 8 == z + 8, pltpu.roll(phases, 68 + 8 * z, 1), packed)
    pack[...] = packed.astype(BF16)
    pl.semaphore_wait(barrier, len(wide))

    z_from = {1: pl.ds(8, 3), -1: pl.ds(3, 3), 0: own_planes}
    z_to = {1: pl.ds(0, 3), -1: pl.ds(11, 3), 0: own_planes}
    z2_from = {1: pl.ds(9, 2), -1: pl.ds(3, 2), 0: own_planes}
    z2_to = {1: pl.ds(1, 2), -1: pl.ds(11, 2), 0: own_planes}
    x_from = {1: pl.ds(PAD + NX - 16, 16), -1: pl.ds(PAD, 16), 0: own_rows}
    x_to = {1: pl.ds(0, 16), -1: pl.ds(PAD + NX, 16), 0: own_rows}
    q_from = {1: pl.ds(NX - 16, 16), -1: pl.ds(0, 16), 0: pl.ds(0, NX)}
    copies = []
    for dz, dx, dy in halo_offsets():
        if dy == 0 and dx == 0:
            src = edge.at[z_from[dz], :, own_rows, :]
            dst = edge.at[z_to[dz], :, own_rows, :]
        elif dy == 0:
            src = edge.at[z2_from[dz], :, x_from[dx], :]
            dst = edge.at[z2_to[dz], :, x_to[dx], :]
        else:
            src = pack.at[q_from[dx], :]
            dst = (left if dy == 1 else right).at[1 - dz, x_to[dx], :]
        copy = pltpu.make_async_remote_copy(
            src_ref=src, dst_ref=dst, send_sem=hs.at[0], recv_sem=hr.at[0 if dz == 0 else 1],
            device_id=device(dz, dx, dy), device_id_type=MESH,
        )
        copies.append((abs(dz) + abs(dx) + abs(dy), dz == 0, copy))
    for distance in (1, 2, 3):
        if distance == 3:
            greet(ready.at[0], near)
            pl.semaphore_wait(ready.at[0], len(near))
        for late in (False, True):
            for length, flat, copy in copies:
                if length == distance and flat == late:
                    copy.start()
    greet(ready.at[2], far)

    def settle(semaphore, ref):
        pltpu.make_async_copy(ref, ref, semaphore).wait()

    def arrived(late):
        settle(hr.at[late], v0.at[pl.ds(0, 11), 0, pl.ds(0, 64 if late else 32), :])

    half = lax.broadcasted_iota(jnp.int32, (1, NY), 1)
    low = lax.rem(half, 8) < 4
    first, last = half == 0, half == NY - 1

    def fill(side, base, count):
        joined = jnp.where(
            low, left[side].astype(F32)[LO:HI], right[side].astype(F32)[LO:HI]
        )

        halves = HALF_GAS + HALF_STEP * joined

        def body(i, _):
            z = base + i
            turn = i + NZ - 3 if side == 0 else i
            v0[z, 0, R, :] = edge[z, 0].astype(F32)[LO:HI]
            mk[z, 0, R, :] = HALF_GAS + HALF_STEP * edge[z, 1].astype(F32)[LO:HI]
            v0[z, 1, R, :] = pltpu.roll(joined, lax.rem(252 - 8 * turn, 128), 1)
            mk[z, 1, R, :] = pltpu.roll(halves, lax.rem(188 - 8 * turn, 128), 1)
            return 0

        lax.fori_loop(0, count, body, 0, unroll=True)

    def ahead(main, side):
        a, b = pltpu.roll(main, NY - 1, 2), pltpu.roll(side, NY - 1, 2)
        return jnp.where(last, b, a), jnp.where(last, a, b)

    def behind(main, side):
        a, b = pltpu.roll(main, 1, 2), pltpu.roll(side, 1, 2)
        return jnp.where(first, b, a), jnp.where(first, a, b)

    def weight(a, b):
        return 1.0 / (a + b)

    def owned(z, values):
        total = None
        for k in range(values.shape[0]):
            scale = jnp.where((z + k >= 3) & (z + k < 11), 1.0, 0.0).astype(F32)
            term = scale * values[k]
            total = term if total is None else total + term
        return total

    def weights(z, n, energy, only):
        zs = pl.ds(z, n)
        for a in range(PAD if only else LO, PAD + NX if only else HI, 8):
            rows = slice(a, a + 8)
            column = [mk[pl.ds(z - 1, n + 2), t, rows, :] for t in (0, 1)]
            here = [c[1:-1] for c in column]
            wy_now = [weight(p, q) for p, q in zip(here, ahead(*here))]
            wy_back = behind(*wy_now)
            for t in (0,) if only else (0, 1):
                across = weight(column[t][1:], column[t][:-1])
                wx_now = weight(here[t], mk[zs, t, a + 1 : a + 9, :])
                wx_back = weight(here[t], mk[zs, t, a - 1 : a + 7, :])
                total = mass_shift + across[1:] + across[:-1] + wx_now + wx_back
                total = total + wy_now[t] + wy_back[t]
                wz[pl.ds(z - 1, n + 1), t, rows, :] = across
                wx[zs, t, rows, :] = wx_now
                if only and a == PAD:
                    wx[zs, t, pl.ds(PAD - 8, 8), :] = weight(
                        mk[zs, t, pl.ds(PAD - 8, 8), :], mk[zs, t, pl.ds(PAD - 7, 8), :]
                    )
                wy[zs, t, rows, :] = wy_now[t]
                wb[zs, t, rows, :] = wy_back[t]
                di[zs, t, rows, :] = 1.0 / total
                if t == 0 and not only and PAD <= a < PAD + NX:
                    v = v0[zs, 0, rows, :]
                    energy = energy + owned(z, v * v * total)
        return energy

    def stencil(field, result, z, n, sums, only):
        zs = pl.ds(z, n)
        for a in range(PAD if only else LO, PAD + NX if only else HI, 8):
            rows, up, down = slice(a, a + 8), slice(a + 1, a + 9), slice(a - 1, a + 7)
            column = [field[pl.ds(z - 1, n + 2), t, rows, :] for t in (0, 1)]
            here = [c[1:-1] for c in column]
            after, before = ahead(*here), behind(*here)
            for t in (0,) if only else (0, 1):
                v, across = here[t], wz[pl.ds(z - 1, n + 1), t, rows, :]
                total = mass_shift * v + wy[zs, t, rows, :] * (v - after[t])
                total = total + wb[zs, t, rows, :] * (v - before[t])
                total = total + across[1:] * (v - column[t][2:])
                total = total + across[:-1] * (v - column[t][:-2])
                total = total + wx[zs, t, rows, :] * (v - field[zs, t, up, :])
                total = total + wx[zs, t, down, :] * (v - field[zs, t, down, :])
                now = total * di[zs, t, rows, :]
                result[zs, t, rows, :] = now
                if sums is not None and t == 0 and PAD <= a < PAD + NX:
                    sums = (sums[0] + owned(z, v * total), sums[1] + owned(z, now * total))
        return sums

    def at_turn(groups, i):
        return groups[0] + i * (groups[1] - groups[0]) if len(groups) > 1 else groups[0]

    def advance(field, result, groups, n, sums, ends=False, rims=None):
        def body(i, sums):
            if rims is not None:
                stencil(field, result, at_turn(rims, i), 1, None, True)
            return stencil(field, result, at_turn(groups, i), n, sums, ends)

        return lax.fori_loop(0, len(groups), body, sums)

    def lay(groups, n, energy, rims=None):
        def body(i, energy):
            if rims is not None:
                weights(at_turn(rims, i), 1, None, True)
            return weights(at_turn(groups, i), n, energy, False)

        return lax.fori_loop(0, len(groups), body, energy)

    zero = jnp.zeros((8, NY), F32)
    s1 = s2 = s3 = (zero, zero)
    arrived(0)
    fill(1, 3, NZ)
    m0 = lay((4, 7), 3, zero)
    s1 = advance(v0, u1, (4, 7), 3, s1)
    s2 = advance(u1, u2, (5, 7), 2, s2)
    s3 = advance(u2, u3, (6,), 2, s3, True)
    pl.semaphore_wait(ready.at[2], len(far))
    greet(ready.at[3], distant)
    arrived(1)
    fill(0, 0, 3)
    fill(2, 11, 3)
    m0 = lay((2, 10), 2, m0, (1, 12))
    s1 = advance(v0, u1, (2, 10), 2, s1, rims=(1, 12))
    s2 = advance(u1, u2, (3, 9), 2, s2, rims=(2, 11))
    s3 = advance(u2, u3, (3, 8), 3, s3, True)
    (m1, m2), (m3, m4), (m5, _) = s1, s2, s3

    spot = lax.broadcasted_iota(jnp.int32, (1, NY), 1)
    zero_row = jnp.zeros((1, NY), F32)
    row = jnp.zeros((1, NY), F32)
    for k, m in enumerate((m0, m1, m2, m3, m4, m5)):
        row = jnp.where(spot == k, jnp.sum(m, keepdims=True), row)

    def keep(z, _):
        for out, field in ((b1, u1), (b2, u2), (b3, u3)):
            out[z] = field[z + 3, 0, pl.ds(PAD, NX), :]
        return 0

    pl.semaphore_wait(ready.at[3], len(distant))
    place = 0
    plane = [(dz, 0, dy) for dz in range(gz) for dy in range(gy)]
    line = [(0, dx, 0) for dx in range(gx)]
    for turn, group in enumerate((plane, line)):
        group = sorted((o for o in group if o != (0, 0, 0)), key=lambda o: -reach(o))
        n = len(group)
        mine[turn] = row
        for i, offset in enumerate(group):
            pltpu.make_async_remote_copy(
                src_ref=mine.at[turn], dst_ref=got.at[place + i],
                send_sem=rs.at[0], recv_sem=rr.at[turn],
                device_id=device(*offset), device_id_type=MESH,
            ).start()
        if turn == 0:
            lax.fori_loop(0, NZ, keep, 0)
        settle(rr.at[turn], got.at[pl.ds(place, n)])
        pairs = [(row, zero_row)] + [(got[place + i], zero_row) for i in range(min(n, 7))]
        for i in range(7, n):
            high, rest = pairs[i % 8]
            high, error = two_sum(high, got[place + i])
            pairs[i % 8] = (high, rest + error)
        while len(pairs) > 1:
            joined_pairs = []
            for k in range(0, len(pairs) - 1, 2):
                high, error = two_sum(pairs[k][0], pairs[k + 1][0])
                joined_pairs.append((high, error + (pairs[k][1] + pairs[k + 1][1])))
            pairs = joined_pairs + pairs[len(pairs) // 2 * 2 :]
        high, rest = pairs[0]
        row = jnp.where(spot < NY // 2, high, high + pltpu.roll(rest, NY // 2, 1))
        place += n

    def at(k):
        return jnp.sum(jnp.where(spot == k, row, 0.0), axis=1, keepdims=True)

    m = [(at(k), at(k + NY // 2)) for k in range(6)]
    none = jnp.zeros((1, 1), F32)
    scale = (1.0 / m[0][0], none)
    m = [times(quick(*k), scale) for k in m]

    def cross(a, b, c, d):
        return minus(times(a, b), c, d)

    a11, a12 = cross(m[3], m[1], m[2], m[2]), cross(m[4], m[1], m[2], m[3])
    a22 = cross(m[5], m[1], m[3], m[3])
    c1, c2 = cross(m[1], m[1], m[2], m[0]), cross(m[2], m[1], m[3], m[0])
    x2 = cross(c2, a11, c1, a12)[0] / cross(a22, a11, a12, a12)[0]
    x1 = (c1[0] - a12[0] * x2) / a11[0]
    x0 = (m[0][0] - m[2][0] * x1 - m[3][0] * x2) / m[1][0]
    x_poly = [x0, x1, x2]
    z_poly = [jnp.ones((1, 1), F32)] + [-x for x in x_poly]
    for out, c in zip((k0, k1, k2, k3, k4, k5, k6), x_poly + z_poly):
        out[...] = jnp.broadcast_to(c, (1, NY))
    settle(hs.at[0], v0.at[pl.ds(0, 11), 0])
    settle(rs.at[0], got)


def solution(mesh):
    sizes = (mesh.shape["gz"], mesh.shape["gx"], mesh.shape["gy"])
    hops = sizes[0] * sizes[2] + sizes[1] - 2
    field = pltpu.VMEM((14, 2, ROWS, NY), F32)

    def on_device(right_side, phase_mask):
        block = jax.ShapeDtypeStruct((NZ, NX, NY), F32)
        coefficient = jax.ShapeDtypeStruct((1, NY), F32)
        u1, u2, u3, *coef = pl.pallas_call(
            functools.partial(kernel, sizes),
            out_shape=(block,) * 3 + (coefficient,) * 7,
            in_specs=[pl.BlockSpec(memory_space=pltpu.HBM)] * 2,
            out_specs=[pl.BlockSpec(memory_space=pltpu.VMEM)] * 10,
            scratch_shapes=[
                pltpu.VMEM((NZ, NX, NY), jnp.int32),
                pltpu.VMEM((14, 2, ROWS, NY), BF16),
                pltpu.VMEM((NX, NY), BF16),
                pltpu.VMEM((3, ROWS, NY), BF16),
                pltpu.VMEM((3, ROWS, NY), BF16),
                *([field] * 10),
                pltpu.VMEM((2, 1, NY), F32),
                pltpu.VMEM((hops, 1, NY), F32),
                pltpu.SemaphoreType.DMA((2,)),
                pltpu.SemaphoreType.DMA((1,)),
                pltpu.SemaphoreType.DMA((2,)),
                pltpu.SemaphoreType.DMA((1,)),
                pltpu.SemaphoreType.DMA((2,)),
                pltpu.SemaphoreType.REGULAR((4,)),
            ],
            compiler_params=pltpu.CompilerParams(
                collective_id=0, has_side_effects=True, vmem_limit_bytes=24 * 2**20
            ),
        )(*(pltpu.with_memory_space_constraint(a, pltpu.HBM) for a in (right_side, phase_mask)))
        u0 = right_side.astype(F32)
        c = [k[None] for k in coef]
        pressure = c[0] * u0 + c[1] * u1 + c[2] * u2
        return pressure, c[3] * u0 + c[4] * u1 + c[5] * u2 + c[6] * u3

    placed = P("gz", "gx", "gy")
    return jax.shard_map(
        on_device, mesh=mesh, in_specs=(placed, placed), out_specs=(placed, placed), check_vma=False
    )
```

```python
import functools

import jax
import jax.numpy as jnp
from jax import lax
from jax.experimental import pallas as pl
from jax.experimental.pallas import tpu as pltpu
from jax.sharding import PartitionSpec as P

MESH = pl.DeviceIdType.MESH
F32 = jnp.float32
BF16 = jnp.bfloat16

mass_shift = 0.05
HALF_GAS, HALF_STEP = 0.5, 499.5

NZ, NX, NY = 8, 64, 128
PAD = 16
ROWS = NX + 2 * PAD
LO, HI = PAD - 8, PAD + NX + 8
R = slice(LO, HI)
UP, DOWN = slice(LO + 1, HI + 1), slice(LO - 1, HI - 1)
OWN = slice(8, 8 + NX)


def halo_offsets():
    out = []
    for dz in (-1, 0, 1):
        for dx in (-1, 0, 1):
            for dy in (-1, 0, 1):
                if (dz, dx, dy) != (0, 0, 0):
                    out.append((dz, dx, dy))
    return out


def two_sum(a, b):
    s = a + b
    t = s - a
    return s, (a - (s - t)) + (b - t)


def quick(a, b):
    s = a + b
    return s, b - (s - a)


def split(a):
    c = 4097.0 * a
    high = c - (c - a)
    return high, a - high


def times(a, b):
    p = a[0] * b[0]
    (ah, al), (bh, bl) = split(a[0]), split(b[0])
    error = ((ah * bh - p) + ah * bl + al * bh) + al * bl
    return quick(p, error + (a[0] * b[1] + a[1] * b[0]))


def minus(a, b, c):
    p, e = times(b, c)
    s, t = two_sum(a[0], -p)
    return quick(s, t + (a[1] - e))


def kernel(sizes, rhs_hbm, mask_hbm, b1, b2, b3, k0, k1, k2, k3, k4, k5, k6, maskv, edge, pack, left, right,
           v0, mk, wx, wy, wb, wz, di, u1, u2, u3, mine, got, in_sem, hs, hr, rs, rr, ready):
    gz, gx, gy = sizes
    iz, ix, iy = (lax.axis_index(a) for a in ("gz", "gx", "gy"))

    def device(dz, dx, dy):
        return {
            "gz": lax.rem(iz + (dz % gz), gz),
            "gx": lax.rem(ix + (dx % gx), gx),
            "gy": lax.rem(iy + (dy % gy), gy),
        }

    own_rows = pl.ds(PAD, NX)
    own_planes = pl.ds(3, NZ)
    load_mask = pltpu.make_async_copy(mask_hbm, maskv, in_sem.at[0])
    load_rhs = pltpu.make_async_copy(rhs_hbm, edge.at[own_planes, 0, own_rows, :], in_sem.at[1])
    load_mask.start()
    load_rhs.start()

    near = sorted(
        {(o % gz, 0, 0) for o in (1, -1)}
        | {(0, o % gx, 0) for o in (1, -1, 2, -2)}
        | {(0, 0, o % gy) for o in (1, -1)}
        - {(0, 0, 0)}
    )
    far = sorted(
        ({(o % gz, 0, 0) for o in (2, -2)}
        | {(0, o % gx, 0) for o in (4, -4)}
        | {(0, 0, o % gy) for o in (2, -2)})
        - {(0, 0, 0)}
    )

    distant = sorted(({(o % gz, 0, 0) for o in (4, -4)} | {(0, 0, o % gy) for o in (4, -4)}) - {(0, 0, 0)})

    wide = sorted(
        set(near)
        | {
            (dz % gz, dx % gx, dy % gy)
            for dz, dx, dy in halo_offsets()
            if abs(dz) + abs(dx) + abs(dy) <= 2
        }
    )

    def reach(offset):
        return sum(min(o, n - o) for o, n in zip(offset, sizes))

    def greet(semaphore, offsets):
        for offset in offsets:
            pl.semaphore_signal(semaphore, inc=1, device_id=device(*offset), device_id_type=MESH)

    barrier = pltpu.get_barrier_semaphore()
    greet(barrier, sorted(wide, key=lambda o: -reach(o)))

    lane = lax.broadcasted_iota(jnp.int32, (NX, NY), 1)
    load_mask.wait()
    load_rhs.wait()
    edge[own_planes, 1, own_rows, :] = maskv[...].astype(F32).astype(BF16)
    packed = jnp.zeros((NX, NY), F32)
    for z in range(NZ):
        values = edge[3 + z, 0, own_rows, :].astype(F32)
        phases = maskv[z].astype(F32)
        packed = jnp.where(lane // 8 == z, pltpu.roll(values, 4 + 8 * z, 1), packed)
        packed = jnp.where(lane // 8 == z + 8, pltpu.roll(phases, 68 + 8 * z, 1), packed)
    pack[...] = packed.astype(BF16)
    pl.semaphore_wait(barrier, len(wide))

    z_from = {1: pl.ds(8, 3), -1: pl.ds(3, 3), 0: own_planes}
    z_to = {1: pl.ds(0, 3), -1: pl.ds(11, 3), 0: own_planes}
    z2_from = {1: pl.ds(9, 2), -1: pl.ds(3, 2), 0: own_planes}
    z2_to = {1: pl.ds(1, 2), -1: pl.ds(11, 2), 0: own_planes}
    x_from = {1: pl.ds(PAD + NX - 16, 16), -1: pl.ds(PAD, 16), 0: own_rows}
    x_to = {1: pl.ds(0, 16), -1: pl.ds(PAD + NX, 16), 0: own_rows}
    q_from = {1: pl.ds(NX - 16, 16), -1: pl.ds(0, 16), 0: pl.ds(0, NX)}
    copies = []
    for dz, dx, dy in halo_offsets():
        if dy == 0 and dx == 0:
            src = edge.at[z_from[dz], :, own_rows, :]
            dst = edge.at[z_to[dz], :, own_rows, :]
        elif dy == 0:
            src = edge.at[z2_from[dz], :, x_from[dx], :]
            dst = edge.at[z2_to[dz], :, x_to[dx], :]
        else:
            src = pack.at[q_from[dx], :]
            dst = (left if dy == 1 else right).at[1 - dz, x_to[dx], :]
        copy = pltpu.make_async_remote_copy(
            src_ref=src, dst_ref=dst, send_sem=hs.at[0], recv_sem=hr.at[0 if dz == 0 else 1],
            device_id=device(dz, dx, dy), device_id_type=MESH,
        )
        copies.append((abs(dz) + abs(dx) + abs(dy), dz == 0, copy))
    for distance in (1, 2, 3):
        if distance == 3:
            greet(ready.at[0], near)
            pl.semaphore_wait(ready.at[0], len(near))
        for late in (False, True):
            for length, flat, copy in copies:
                if length == distance and flat == late:
                    copy.start()
    greet(ready.at[2], far)

    def settle(semaphore, ref):
        pltpu.make_async_copy(ref, ref, semaphore).wait()

    def arrived(late):
        settle(hr.at[late], v0.at[pl.ds(0, 11), 0, pl.ds(0, 64 if late else 32), :])

    half = lax.broadcasted_iota(jnp.int32, (1, NY), 1)
    low = lax.rem(half, 8) < 4
    first, last = half == 0, half == NY - 1

    def fill(side, base, count):
        joined = jnp.where(
            low, left[side].astype(F32)[LO:HI], right[side].astype(F32)[LO:HI]
        )

        halves = HALF_GAS + HALF_STEP * joined

        def body(i, _):
            z = base + i
            turn = i + NZ - 3 if side == 0 else i
            v0[z, 0, R, :] = edge[z, 0].astype(F32)[LO:HI]
            mk[z, 0, R, :] = HALF_GAS + HALF_STEP * edge[z, 1].astype(F32)[LO:HI]
            v0[z, 1, R, :] = pltpu.roll(joined, lax.rem(252 - 8 * turn, 128), 1)
            mk[z, 1, R, :] = pltpu.roll(halves, lax.rem(188 - 8 * turn, 128), 1)
            return 0

        lax.fori_loop(0, count, body, 0, unroll=True)

    def ahead(main, side):
        a, b = pltpu.roll(main, NY - 1, 2), pltpu.roll(side, NY - 1, 2)
        return jnp.where(last, b, a), jnp.where(last, a, b)

    def behind(main, side):
        a, b = pltpu.roll(main, 1, 2), pltpu.roll(side, 1, 2)
        return jnp.where(first, b, a), jnp.where(first, a, b)

    def beside(main, side):
        return (
            [pltpu.roll(jnp.where(first, side, main), NY - 1, 2)],
            [pltpu.roll(jnp.where(last, side, main), 1, 2)],
        )

    def weight(a, b):
        return 1.0 / (a + b)

    def owned(z, values):
        total = None
        for k in range(values.shape[0]):
            scale = jnp.where((z + k >= 3) & (z + k < 11), 1.0, 0.0).astype(F32)
            term = scale * values[k]
            total = term if total is None else total + term
        return total

    def weights(z, n, energy, only):
        zs = pl.ds(z, n)
        for a in range(PAD if only else LO, PAD + NX if only else HI, 8):
            rows = slice(a, a + 8)
            column = [mk[pl.ds(z - 1, n + 2), t, rows, :] for t in (0, 1)]
            here = [c[1:-1] for c in column]
            if only:
                wy_now, wy_back = ([weight(here[0], q[0])] for q in beside(*here))
            else:
                wy_now = [weight(p, q) for p, q in zip(here, ahead(*here))]
                wy_back = behind(*wy_now)
            for t in (0,) if only else (0, 1):
                across = weight(column[t][1:], column[t][:-1])
                wx_now = weight(here[t], mk[zs, t, a + 1 : a + 9, :])
                wx_back = weight(here[t], mk[zs, t, a - 1 : a + 7, :])
                total = mass_shift + across[1:] + across[:-1] + wx_now + wx_back
                total = total + wy_now[t] + wy_back[t]
                wz[pl.ds(z - 1, n + 1), t, rows, :] = across
                wx[zs, t, rows, :] = wx_now
                if only and a == PAD:
                    wx[zs, t, pl.ds(PAD - 8, 8), :] = weight(
                        mk[zs, t, pl.ds(PAD - 8, 8), :], mk[zs, t, pl.ds(PAD - 7, 8), :]
                    )
                wy[zs, t, rows, :] = wy_now[t]
                wb[zs, t, rows, :] = wy_back[t]
                di[zs, t, rows, :] = 1.0 / total
                if t == 0 and not only and PAD <= a < PAD + NX:
                    v = v0[zs, 0, rows, :]
                    energy = energy + owned(z, v * v * total)
        return energy

    def stencil(field, result, z, n, sums, only):
        zs = pl.ds(z, n)
        for a in range(PAD if only else LO, PAD + NX if only else HI, 8):
            rows, up, down = slice(a, a + 8), slice(a + 1, a + 9), slice(a - 1, a + 7)
            column = [field[pl.ds(z - 1, n + 2), t, rows, :] for t in (0, 1)]
            here = [c[1:-1] for c in column]
            after, before = beside(*here) if only else (ahead(*here), behind(*here))
            for t in (0,) if only else (0, 1):
                v, across = here[t], wz[pl.ds(z - 1, n + 1), t, rows, :]
                total = mass_shift * v + wy[zs, t, rows, :] * (v - after[t])
                total = total + wb[zs, t, rows, :] * (v - before[t])
                total = total + across[1:] * (v - column[t][2:])
                total = total + across[:-1] * (v - column[t][:-2])
                total = total + wx[zs, t, rows, :] * (v - field[zs, t, up, :])
                total = total + wx[zs, t, down, :] * (v - field[zs, t, down, :])
                now = total * di[zs, t, rows, :]
                result[zs, t, rows, :] = now
                if sums is not None and t == 0 and PAD <= a < PAD + NX:
                    sums = (sums[0] + owned(z, v * total), sums[1] + owned(z, now * total))
        return sums

    def at_turn(groups, i):
        return groups[0] + i * (groups[1] - groups[0]) if len(groups) > 1 else groups[0]

    def advance(field, result, groups, n, sums, ends=False, rims=None):
        def body(i, sums):
            if rims is not None:
                stencil(field, result, at_turn(rims, i), 1, None, True)
            return stencil(field, result, at_turn(groups, i), n, sums, ends)

        return lax.fori_loop(0, len(groups), body, sums)

    def lay(groups, n, energy, rims=None):
        def body(i, energy):
            if rims is not None:
                weights(at_turn(rims, i), 1, None, True)
            return weights(at_turn(groups, i), n, energy, False)

        return lax.fori_loop(0, len(groups), body, energy)

    zero = jnp.zeros((8, NY), F32)
    s1 = s2 = s3 = (zero, zero)
    arrived(0)
    pl.semaphore_wait(ready.at[2], len(far))
    greet(ready.at[3], distant)
    fill(1, 3, NZ)
    m0 = lay((4, 7), 3, zero)
    s1 = advance(v0, u1, (4, 7), 3, s1)
    s2 = advance(u1, u2, (5, 7), 2, s2)
    s3 = advance(u2, u3, (6,), 2, s3, True)
    arrived(1)
    fill(0, 0, 3)
    fill(2, 11, 3)
    m0 = lay((2, 10), 2, m0, (1, 12))
    s1 = advance(v0, u1, (2, 10), 2, s1, rims=(1, 12))
    s2 = advance(u1, u2, (3, 9), 2, s2, rims=(2, 11))
    s3 = advance(u2, u3, (3, 8), 3, s3, True)
    (m1, m2), (m3, m4), (m5, _) = s1, s2, s3

    spot = lax.broadcasted_iota(jnp.int32, (1, NY), 1)
    zero_row = jnp.zeros((1, NY), F32)
    row = jnp.zeros((1, NY), F32)
    for k, m in enumerate((m0, m1, m2, m3, m4, m5)):
        row = jnp.where(spot == k, jnp.sum(m, keepdims=True), row)

    def keep(z, _):
        for out, field in ((b1, u1), (b2, u2), (b3, u3)):
            out[z] = field[z + 3, 0, pl.ds(PAD, NX), :]
        return 0

    pl.semaphore_wait(ready.at[3], len(distant))
    place = 0
    plane = [(dz, 0, dy) for dz in range(gz) for dy in range(gy)]
    line = [(0, dx, 0) for dx in range(gx)]
    for turn, group in enumerate((plane, line)):
        group = sorted((o for o in group if o != (0, 0, 0)), key=lambda o: -reach(o))
        n = len(group)
        cut = n * 2 // 5 if turn == 0 else 0
        mine[turn] = row
        for i, offset in enumerate(group):
            if turn == 0 and i == cut:
                lax.fori_loop(0, NZ, keep, 0)
            pltpu.make_async_remote_copy(
                src_ref=mine.at[turn], dst_ref=got.at[place + i],
                send_sem=rs.at[0], recv_sem=rr.at[2 * turn + (i < cut)],
                device_id=device(*offset), device_id_type=MESH,
            ).start()
        pairs = [(row, zero_row)]
        for kind, start, stop in ((0, cut, n), (1, 0, cut)):
            if start == stop:
                continue
            settle(rr.at[2 * turn + kind], got.at[pl.ds(place + start, stop - start)])
            for i in range(start, stop):
                if len(pairs) < 8:
                    pairs.append((got[place + i], zero_row))
                    continue
                high, rest = pairs[i % 8]
                high, error = two_sum(high, got[place + i])
                pairs[i % 8] = (high, rest + error)
        while len(pairs) > 1:
            joined_pairs = []
            for k in range(0, len(pairs) - 1, 2):
                high, error = two_sum(pairs[k][0], pairs[k + 1][0])
                joined_pairs.append((high, error + (pairs[k][1] + pairs[k + 1][1])))
            pairs = joined_pairs + pairs[len(pairs) // 2 * 2 :]
        high, rest = pairs[0]
        row = jnp.where(spot < NY // 2, high, high + pltpu.roll(rest, NY // 2, 1))
        place += n

    def at(k):
        return jnp.sum(jnp.where(spot == k, row, 0.0), axis=1, keepdims=True)

    m = [(at(k), at(k + NY // 2)) for k in range(6)]
    none = jnp.zeros((1, 1), F32)
    scale = (1.0 / m[0][0], none)
    m = [times(quick(*k), scale) for k in m]

    def cross(a, b, c, d):
        return minus(times(a, b), c, d)

    a11, a12 = cross(m[3], m[1], m[2], m[2]), cross(m[4], m[1], m[2], m[3])
    a22 = cross(m[5], m[1], m[3], m[3])
    c1, c2 = cross(m[1], m[1], m[2], m[0]), cross(m[2], m[1], m[3], m[0])
    x2 = cross(c2, a11, c1, a12)[0] / cross(a22, a11, a12, a12)[0]
    x1 = (c1[0] - a12[0] * x2) / a11[0]
    x0 = (m[0][0] - m[2][0] * x1 - m[3][0] * x2) / m[1][0]
    x_poly = [x0, x1, x2]
    z_poly = [jnp.ones((1, 1), F32)] + [-x for x in x_poly]
    for out, c in zip((k0, k1, k2, k3, k4, k5, k6), x_poly + z_poly):
        out[...] = jnp.broadcast_to(c, (1, NY))
    settle(hs.at[0], v0.at[pl.ds(0, 11), 0])
    settle(rs.at[0], got)


def solution(mesh):
    sizes = (mesh.shape["gz"], mesh.shape["gx"], mesh.shape["gy"])
    hops = sizes[0] * sizes[2] + sizes[1] - 2
    field = pltpu.VMEM((14, 2, ROWS, NY), F32)

    def on_device(right_side, phase_mask):
        block = jax.ShapeDtypeStruct((NZ, NX, NY), F32)
        coefficient = jax.ShapeDtypeStruct((1, NY), F32)
        u1, u2, u3, *coef = pl.pallas_call(
            functools.partial(kernel, sizes),
            out_shape=(block,) * 3 + (coefficient,) * 7,
            in_specs=[pl.BlockSpec(memory_space=pltpu.HBM)] * 2,
            out_specs=[pl.BlockSpec(memory_space=pltpu.VMEM)] * 10,
            scratch_shapes=[
                pltpu.VMEM((NZ, NX, NY), jnp.int32),
                pltpu.VMEM((14, 2, ROWS, NY), BF16),
                pltpu.VMEM((NX, NY), BF16),
                pltpu.VMEM((3, ROWS, NY), BF16),
                pltpu.VMEM((3, ROWS, NY), BF16),
                *([field] * 10),
                pltpu.VMEM((2, 1, NY), F32),
                pltpu.VMEM((hops, 1, NY), F32),
                pltpu.SemaphoreType.DMA((2,)),
                pltpu.SemaphoreType.DMA((1,)),
                pltpu.SemaphoreType.DMA((2,)),
                pltpu.SemaphoreType.DMA((1,)),
                pltpu.SemaphoreType.DMA((3,)),
                pltpu.SemaphoreType.REGULAR((4,)),
            ],
            compiler_params=pltpu.CompilerParams(
                collective_id=0, has_side_effects=True, vmem_limit_bytes=24 * 2**20
            ),
        )(*(pltpu.with_memory_space_constraint(a, pltpu.HBM) for a in (right_side, phase_mask)))
        u0 = right_side.astype(F32)
        c = [k[None] for k in coef]
        pressure = c[0] * u0 + c[1] * u1 + c[2] * u2
        return pressure, c[3] * u0 + c[4] * u1 + c[5] * u2 + c[6] * u3

    placed = P("gz", "gx", "gy")
    return jax.shard_map(
        on_device, mesh=mesh, in_specs=(placed, placed), out_specs=(placed, placed), check_vma=False
    )
```

```python
import functools

import jax
import jax.numpy as jnp
from jax import lax
from jax.experimental import pallas as pl
from jax.experimental.pallas import tpu as pltpu
from jax.sharding import PartitionSpec as P

MESH = pl.DeviceIdType.MESH
F32 = jnp.float32
BF16 = jnp.bfloat16

mass_shift = 0.05
HALF_GAS, HALF_STEP = 0.5, 499.5

NZ, NX, NY = 8, 64, 128
PAD = 16
ROWS = NX + 2 * PAD
LO, HI = PAD - 8, PAD + NX + 8
R = slice(LO, HI)
UP, DOWN = slice(LO + 1, HI + 1), slice(LO - 1, HI - 1)
OWN = slice(8, 8 + NX)


def halo_offsets():
    out = []
    for dz in (-1, 0, 1):
        for dx in (-1, 0, 1):
            for dy in (-1, 0, 1):
                if (dz, dx, dy) != (0, 0, 0):
                    out.append((dz, dx, dy))
    return out


def two_sum(a, b):
    s = a + b
    t = s - a
    return s, (a - (s - t)) + (b - t)


def quick(a, b):
    s = a + b
    return s, b - (s - a)


def split(a):
    c = 4097.0 * a
    high = c - (c - a)
    return high, a - high


def times(a, b):
    p = a[0] * b[0]
    (ah, al), (bh, bl) = split(a[0]), split(b[0])
    error = ((ah * bh - p) + ah * bl + al * bh) + al * bl
    return quick(p, error + (a[0] * b[1] + a[1] * b[0]))


def minus(a, b, c):
    p, e = times(b, c)
    s, t = two_sum(a[0], -p)
    return quick(s, t + (a[1] - e))


def kernel(sizes, rhs_hbm, mask_hbm, b1, b2, b3, k0, k1, k2, k3, k4, k5, k6, maskv, edge, pack, left, right,
           v0, mk, wx, wy, wb, wz, di, u1, u2, u3, mine, got, in_sem, hs, hr, rs, rr, ready):
    gz, gx, gy = sizes
    iz, ix, iy = (lax.axis_index(a) for a in ("gz", "gx", "gy"))

    def device(dz, dx, dy):
        return {
            "gz": lax.rem(iz + (dz % gz), gz),
            "gx": lax.rem(ix + (dx % gx), gx),
            "gy": lax.rem(iy + (dy % gy), gy),
        }

    own_rows = pl.ds(PAD, NX)
    own_planes = pl.ds(3, NZ)
    load_mask = pltpu.make_async_copy(mask_hbm, maskv, in_sem.at[0])
    load_rhs = pltpu.make_async_copy(rhs_hbm, edge.at[own_planes, 0, own_rows, :], in_sem.at[1])
    load_mask.start()
    load_rhs.start()

    near = sorted(
        {(o % gz, 0, 0) for o in (1, -1)}
        | {(0, o % gx, 0) for o in (1, -1, 2, -2)}
        | {(0, 0, o % gy) for o in (1, -1)}
        - {(0, 0, 0)}
    )
    far = sorted(
        ({(o % gz, 0, 0) for o in (2, -2)}
        | {(0, o % gx, 0) for o in (4, -4)}
        | {(0, 0, o % gy) for o in (2, -2)})
        - {(0, 0, 0)}
    )

    distant = sorted(({(o % gz, 0, 0) for o in (4, -4)} | {(0, 0, o % gy) for o in (4, -4)}) - {(0, 0, 0)})

    wide = sorted(
        set(near)
        | {
            (dz % gz, dx % gx, dy % gy)
            for dz, dx, dy in halo_offsets()
            if abs(dz) + abs(dx) + abs(dy) <= 2
        }
    )

    def reach(offset):
        return sum(min(o, n - o) for o, n in zip(offset, sizes))

    def greet(semaphore, offsets):
        for offset in offsets:
            pl.semaphore_signal(semaphore, inc=1, device_id=device(*offset), device_id_type=MESH)

    barrier = pltpu.get_barrier_semaphore()
    greet(barrier, sorted(wide, key=lambda o: -reach(o)))

    lane = lax.broadcasted_iota(jnp.int32, (NX, NY), 1)
    load_mask.wait()
    load_rhs.wait()
    edge[own_planes, 1, own_rows, :] = maskv[...].astype(F32).astype(BF16)
    packed = jnp.zeros((NX, NY), F32)
    for z in range(NZ):
        values = edge[3 + z, 0, own_rows, :].astype(F32)
        phases = maskv[z].astype(F32)
        packed = jnp.where(lane // 8 == z, pltpu.roll(values, 4 + 8 * z, 1), packed)
        packed = jnp.where(lane // 8 == z + 8, pltpu.roll(phases, 68 + 8 * z, 1), packed)
    pack[...] = packed.astype(BF16)
    pl.semaphore_wait(barrier, len(wide))

    z_from = {1: pl.ds(8, 3), -1: pl.ds(3, 3), 0: own_planes}
    z_to = {1: pl.ds(0, 3), -1: pl.ds(11, 3), 0: own_planes}
    z2_from = {1: pl.ds(9, 2), -1: pl.ds(3, 2), 0: own_planes}
    z2_to = {1: pl.ds(1, 2), -1: pl.ds(11, 2), 0: own_planes}
    x_from = {1: pl.ds(PAD + NX - 16, 16), -1: pl.ds(PAD, 16), 0: own_rows}
    x_to = {1: pl.ds(0, 16), -1: pl.ds(PAD + NX, 16), 0: own_rows}
    q_from = {1: pl.ds(NX - 16, 16), -1: pl.ds(0, 16), 0: pl.ds(0, NX)}
    copies = []
    for dz, dx, dy in halo_offsets():
        if dy == 0 and dx == 0:
            src = edge.at[z_from[dz], :, own_rows, :]
            dst = edge.at[z_to[dz], :, own_rows, :]
        elif dy == 0:
            src = edge.at[z2_from[dz], :, x_from[dx], :]
            dst = edge.at[z2_to[dz], :, x_to[dx], :]
        else:
            src = pack.at[q_from[dx], :]
            dst = (left if dy == 1 else right).at[1 - dz, x_to[dx], :]
        copy = pltpu.make_async_remote_copy(
            src_ref=src, dst_ref=dst, send_sem=hs.at[0], recv_sem=hr.at[0 if dz == 0 else 1],
            device_id=device(dz, dx, dy), device_id_type=MESH,
        )
        copies.append((abs(dz) + abs(dx) + abs(dy), dz == 0, copy))
    for distance in (1, 2, 3):
        if distance == 3:
            greet(ready.at[0], near)
            pl.semaphore_wait(ready.at[0], len(near))
        for late in (False, True):
            for length, flat, copy in copies:
                if length == distance and flat == late:
                    copy.start()
    greet(ready.at[2], far)

    def settle(semaphore, ref):
        pltpu.make_async_copy(ref, ref, semaphore).wait()

    def arrived(late):
        settle(hr.at[late], v0.at[pl.ds(0, 11), 0, pl.ds(0, 64 if late else 32), :])

    half = lax.broadcasted_iota(jnp.int32, (1, NY), 1)
    low = lax.rem(half, 8) < 4
    first, last = half == 0, half == NY - 1

    def fill(side, base, count):
        joined = jnp.where(
            low, left[side].astype(F32)[LO:HI], right[side].astype(F32)[LO:HI]
        )

        halves = HALF_GAS + HALF_STEP * joined

        def body(i, _):
            z = base + i
            turn = i + NZ - 3 if side == 0 else i
            v0[z, 0, R, :] = edge[z, 0].astype(F32)[LO:HI]
            mk[z, 0, R, :] = HALF_GAS + HALF_STEP * edge[z, 1].astype(F32)[LO:HI]
            v0[z, 1, R, :] = pltpu.roll(joined, lax.rem(252 - 8 * turn, 128), 1)
            mk[z, 1, R, :] = pltpu.roll(halves, lax.rem(188 - 8 * turn, 128), 1)
            return 0

        lax.fori_loop(0, count, body, 0, unroll=True)

    def ahead(main, side):
        a, b = pltpu.roll(main, NY - 1, 2), pltpu.roll(side, NY - 1, 2)
        return jnp.where(last, b, a), jnp.where(last, a, b)

    def behind(main, side):
        a, b = pltpu.roll(main, 1, 2), pltpu.roll(side, 1, 2)
        return jnp.where(first, b, a), jnp.where(first, a, b)

    def beside(main, side):
        return (
            [pltpu.roll(jnp.where(first, side, main), NY - 1, 2)],
            [pltpu.roll(jnp.where(last, side, main), 1, 2)],
        )

    def weight(a, b):
        return 1.0 / (a + b)

    def owned(z, values):
        total = None
        for k in range(values.shape[0]):
            scale = jnp.where((z + k >= 3) & (z + k < 11), 1.0, 0.0).astype(F32)
            term = scale * values[k]
            total = term if total is None else total + term
        return total

    def weights(z, n, energy, only):
        zs = pl.ds(z, n)
        for a in range(PAD if only else LO, PAD + NX if only else HI, 8):
            rows = slice(a, a + 8)
            column = [mk[pl.ds(z - 1, n + 2), t, rows, :] for t in (0, 1)]
            here = [c[1:-1] for c in column]
            if only:
                wy_now, wy_back = ([weight(here[0], q[0])] for q in beside(*here))
            else:
                wy_now = [weight(p, q) for p, q in zip(here, ahead(*here))]
                wy_back = behind(*wy_now)
            for t in (0,) if only else (0, 1):
                across = weight(column[t][1:], column[t][:-1])
                wx_now = weight(here[t], mk[zs, t, a + 1 : a + 9, :])
                wx_back = weight(here[t], mk[zs, t, a - 1 : a + 7, :])
                total = mass_shift + across[1:] + across[:-1] + wx_now + wx_back
                total = total + wy_now[t] + wy_back[t]
                wz[pl.ds(z - 1, n + 1), t, rows, :] = across
                wx[zs, t, rows, :] = wx_now
                if only and a == PAD:
                    wx[zs, t, pl.ds(PAD - 8, 8), :] = weight(
                        mk[zs, t, pl.ds(PAD - 8, 8), :], mk[zs, t, pl.ds(PAD - 7, 8), :]
                    )
                wy[zs, t, rows, :] = wy_now[t]
                wb[zs, t, rows, :] = wy_back[t]
                di[zs, t, rows, :] = 1.0 / total
                if t == 0 and not only and PAD <= a < PAD + NX:
                    v = v0[zs, 0, rows, :]
                    energy = energy + owned(z, v * v * total)
        return energy

    def stencil(field, result, z, n, sums, only):
        zs = pl.ds(z, n)
        for a in range(PAD if only else LO, PAD + NX if only else HI, 8):
            rows, up, down = slice(a, a + 8), slice(a + 1, a + 9), slice(a - 1, a + 7)
            column = [field[pl.ds(z - 1, n + 2), t, rows, :] for t in (0, 1)]
            here = [c[1:-1] for c in column]
            after, before = beside(*here) if only else (ahead(*here), behind(*here))
            for t in (0,) if only else (0, 1):
                v, across = here[t], wz[pl.ds(z - 1, n + 1), t, rows, :]
                total = mass_shift * v + wy[zs, t, rows, :] * (v - after[t])
                total = total + wb[zs, t, rows, :] * (v - before[t])
                total = total + across[1:] * (v - column[t][2:])
                total = total + across[:-1] * (v - column[t][:-2])
                total = total + wx[zs, t, rows, :] * (v - field[zs, t, up, :])
                total = total + wx[zs, t, down, :] * (v - field[zs, t, down, :])
                now = total * di[zs, t, rows, :]
                result[zs, t, rows, :] = now
                if sums is not None and t == 0 and PAD <= a < PAD + NX:
                    sums = (sums[0] + owned(z, v * total), sums[1] + owned(z, now * total))
        return sums

    def at_turn(groups, i):
        return groups[0] + i * (groups[1] - groups[0]) if len(groups) > 1 else groups[0]

    def advance(field, result, groups, n, sums, ends=False, rims=None):
        def body(i, sums):
            if rims is not None:
                stencil(field, result, at_turn(rims, i), 1, None, True)
            return stencil(field, result, at_turn(groups, i), n, sums, ends)

        return lax.fori_loop(0, len(groups), body, sums)

    def lay(groups, n, energy, rims=None):
        def body(i, energy):
            if rims is not None:
                weights(at_turn(rims, i), 1, None, True)
            return weights(at_turn(groups, i), n, energy, False)

        return lax.fori_loop(0, len(groups), body, energy)

    zero = jnp.zeros((8, NY), F32)
    s1 = s2 = s3 = (zero, zero)
    arrived(0)
    pl.semaphore_wait(ready.at[2], len(far))
    greet(ready.at[3], distant)
    fill(1, 3, NZ)
    m0 = lay((4, 7), 3, zero)
    s1 = advance(v0, u1, (4, 7), 3, s1)
    s2 = advance(u1, u2, (5, 7), 2, s2)
    s3 = advance(u2, u3, (6,), 2, s3, True)
    arrived(1)
    fill(0, 0, 3)
    fill(2, 11, 3)
    m0 = lay((2, 10), 2, m0, (1, 12))
    s1 = advance(v0, u1, (2, 10), 2, s1, rims=(1, 12))
    s2 = advance(u1, u2, (3, 9), 2, s2, rims=(2, 11))
    s3 = advance(u2, u3, (3, 8), 3, s3, True)
    (m1, m2), (m3, m4), (m5, _) = s1, s2, s3

    spot = lax.broadcasted_iota(jnp.int32, (1, NY), 1)
    zero_row = jnp.zeros((1, NY), F32)
    row = jnp.zeros((1, NY), F32)
    for k, m in enumerate((m0, m1, m2, m3, m4, m5)):
        row = jnp.where(spot == k, jnp.sum(m, keepdims=True), row)

    def keep(z, _):
        for out, field in ((b1, u1), (b2, u2), (b3, u3)):
            out[z] = field[z + 3, 0, pl.ds(PAD, NX), :]
        return 0

    place = 0
    plane = [(dz, 0, dy) for dz in range(gz) for dy in range(gy)]
    line = [(0, dx, 0) for dx in range(gx)]
    for turn, group in enumerate((line, plane)):
        group = sorted((o for o in group if o != (0, 0, 0)), key=lambda o: -reach(o))
        n = len(group)
        cut = n * 2 // 5 if turn == 1 else 0
        mine[turn] = row
        if turn == 1:
            pl.semaphore_wait(ready.at[3], len(distant))
        for i, offset in enumerate(group):
            pltpu.make_async_remote_copy(
                src_ref=mine.at[turn], dst_ref=got.at[place + i],
                send_sem=rs.at[0], recv_sem=rr.at[turn + (i < cut)],
                device_id=device(*offset), device_id_type=MESH,
            ).start()
        if turn == 0:
            lax.fori_loop(0, NZ, keep, 0)
        pairs = [(row, zero_row)]
        for kind, start, stop in ((0, cut, n), (1, 0, cut)):
            if start == stop:
                continue
            settle(rr.at[turn + kind], got.at[pl.ds(place + start, stop - start)])
            for i in range(start, stop):
                if len(pairs) < 8:
                    pairs.append((got[place + i], zero_row))
                    continue
                high, rest = pairs[i % 8]
                high, error = two_sum(high, got[place + i])
                pairs[i % 8] = (high, rest + error)
        while len(pairs) > 1:
            joined_pairs = []
            for k in range(0, len(pairs) - 1, 2):
                high, error = two_sum(pairs[k][0], pairs[k + 1][0])
                joined_pairs.append((high, error + (pairs[k][1] + pairs[k + 1][1])))
            pairs = joined_pairs + pairs[len(pairs) // 2 * 2 :]
        high, rest = pairs[0]
        row = jnp.where(spot < NY // 2, high, high + pltpu.roll(rest, NY // 2, 1))
        place += n

    def at(k):
        return jnp.sum(jnp.where(spot == k, row, 0.0), axis=1, keepdims=True)

    m = [(at(k), at(k + NY // 2)) for k in range(6)]
    none = jnp.zeros((1, 1), F32)
    scale = (1.0 / m[0][0], none)
    m = [times(quick(*k), scale) for k in m]

    def cross(a, b, c, d):
        return minus(times(a, b), c, d)

    a11, a12 = cross(m[3], m[1], m[2], m[2]), cross(m[4], m[1], m[2], m[3])
    a22 = cross(m[5], m[1], m[3], m[3])
    c1, c2 = cross(m[1], m[1], m[2], m[0]), cross(m[2], m[1], m[3], m[0])
    x2 = cross(c2, a11, c1, a12)[0] / cross(a22, a11, a12, a12)[0]
    x1 = (c1[0] - a12[0] * x2) / a11[0]
    x0 = (m[0][0] - m[2][0] * x1 - m[3][0] * x2) / m[1][0]
    x_poly = [x0, x1, x2]
    z_poly = [jnp.ones((1, 1), F32)] + [-x for x in x_poly]
    for out, c in zip((k0, k1, k2, k3, k4, k5, k6), x_poly + z_poly):
        out[...] = jnp.broadcast_to(c, (1, NY))
    settle(hs.at[0], v0.at[pl.ds(0, 11), 0])
    settle(rs.at[0], got)


def solution(mesh):
    sizes = (mesh.shape["gz"], mesh.shape["gx"], mesh.shape["gy"])
    hops = sizes[0] * sizes[2] + sizes[1] - 2
    field = pltpu.VMEM((14, 2, ROWS, NY), F32)

    def on_device(right_side, phase_mask):
        block = jax.ShapeDtypeStruct((NZ, NX, NY), F32)
        coefficient = jax.ShapeDtypeStruct((1, NY), F32)
        u1, u2, u3, *coef = pl.pallas_call(
            functools.partial(kernel, sizes),
            out_shape=(block,) * 3 + (coefficient,) * 7,
            in_specs=[pl.BlockSpec(memory_space=pltpu.HBM)] * 2,
            out_specs=[pl.BlockSpec(memory_space=pltpu.VMEM)] * 10,
            scratch_shapes=[
                pltpu.VMEM((NZ, NX, NY), jnp.int32),
                pltpu.VMEM((14, 2, ROWS, NY), BF16),
                pltpu.VMEM((NX, NY), BF16),
                pltpu.VMEM((3, ROWS, NY), BF16),
                pltpu.VMEM((3, ROWS, NY), BF16),
                *([field] * 10),
                pltpu.VMEM((2, 1, NY), F32),
                pltpu.VMEM((hops, 1, NY), F32),
                pltpu.SemaphoreType.DMA((2,)),
                pltpu.SemaphoreType.DMA((1,)),
                pltpu.SemaphoreType.DMA((2,)),
                pltpu.SemaphoreType.DMA((1,)),
                pltpu.SemaphoreType.DMA((3,)),
                pltpu.SemaphoreType.REGULAR((4,)),
            ],
            compiler_params=pltpu.CompilerParams(
                collective_id=0, has_side_effects=True, vmem_limit_bytes=24 * 2**20
            ),
        )(*(pltpu.with_memory_space_constraint(a, pltpu.HBM) for a in (right_side, phase_mask)))
        u0 = right_side.astype(F32)
        c = [k[None] for k in coef]
        pressure = c[0] * u0 + c[1] * u1 + c[2] * u2
        return pressure, c[3] * u0 + c[4] * u1 + c[5] * u2 + c[6] * u3

    placed = P("gz", "gx", "gy")
    return jax.shard_map(
        on_device, mesh=mesh, in_specs=(placed, placed), out_specs=(placed, placed), check_vma=False
    )
```
